256 devices in a mesh: segment: 8 (over y, core), row: 32 (over z, x).
Axes of the slice: x: 4, y: 4, z: 8, core: 2. Of those that a mesh axis runs over, the one named last changes fastest.
Arguments:
- snapshots: float32 [8192, 1024], P('row', 'segment'), may hold values from -6 to 6
- basis: float32 [8192, 4096], P('row', 'segment'), may hold values from -0.0625 to 0.0625
Outputs:
- residual: float32 [8192, 1024], P('row', 'segment')
- coefficients: float32 [4096, 1024], P('segment')
- residual_rms: float32 [1024], P('segment')
The draws below stay inside these ranges and needn't reach their ends.
All inputs are finite; a program needn't handle non-finite values.
Results may differ from the reference program's by a relative error of at most 0.0001.
Values sent between devices are 32-bit elements; how exact they have to be, the bound alone decides.
No kernel may reach another device: no remote copies, remote signals or barrier semaphores. Data moves between devices by JAX's collectives and lax.ppermute only.
A program may use at most 64 MiB of HBM per device.

```python
import jax
import jax.numpy as jnp
from jax import lax

SEC = 512
TICKS = 2
BATCH = 128
ROWS = 8192
BASIS = 4096
COLS = 1024


def steps_of(stream_key, dims, shards, least, largest):
    def one(position, shards_of):
        heights = jax.random.uniform(jax.random.fold_in(jax.random.fold_in(stream_key, 6), position), (shards_of,), jnp.float32, least / len(shards), largest / len(shards))
        return jnp.repeat(jnp.exp(heights), dims[position] // shards_of).reshape((-1,) + (1,) * (len(dims) - position - 1))

    factor_of = one(*shards[0])
    for cut in shards[1:]:
        factor_of = factor_of * one(*cut)
    return factor_of


def noise(key, dims, deviation, most, split=(), kind=jnp.bfloat16):
    values = jax.random.normal(key, dims, jnp.float32) * deviation
    if len(split) > 0:
        values = steps_of(key, dims, split, -0.22, 0.18) * values
    return jnp.clip(values, min=-most, max=most).astype(kind)


def setup_inputs(seed: int = 0) -> dict:
    keys = jax.random.split(jax.random.key(seed), 3)
    return {
        "snapshots": noise(keys[0], (ROWS, COLS), 1.0, 6.0, ((0, 32), (1, 8)), jnp.float32),
        "basis": noise(keys[1], (ROWS, BASIS), ROWS ** -0.5, 0.0625, ((0, 32), (1, 8)), jnp.float32),
    }


def project(part, vec):
    high = lax.Precision.HIGHEST
    first = jnp.dot(part.T, vec, precision=high, preferred_element_type=jnp.float32)
    moved = vec - jnp.dot(part, first, precision=high, preferred_element_type=jnp.float32)
    second = jnp.dot(part.T, moved, precision=high, preferred_element_type=jnp.float32)
    return (moved - jnp.dot(part, second, precision=high, preferred_element_type=jnp.float32), first + second)

def reference(snapshots, basis):
    sections = basis.shape[1] // SEC

    def per_batch(batch_index, carry):
        resid, coeff = carry
        vec = lax.dynamic_slice_in_dim(snapshots, batch_index * BATCH, BATCH, 1)

        def per_section(step, inner):
            vec, coeff = inner
            section = (batch_index + step) % sections
            part = lax.dynamic_slice_in_dim(basis, section * SEC, SEC, 1)
            vec, coef = project(part, vec)
            coeff = lax.dynamic_update_slice(coeff, coef, (section * SEC, batch_index * BATCH))
            return (vec, coeff)
        vec, coeff = lax.fori_loop(jnp.int32(0), jnp.int32(TICKS), per_section, (vec, coeff))
        resid = lax.dynamic_update_slice(resid, vec, (jnp.int32(0), batch_index * BATCH))
        return (resid, coeff)
    resid = jnp.zeros(snapshots.shape, jnp.float32)
    coeff = jnp.zeros((basis.shape[1], snapshots.shape[1]), jnp.float32)
    resid, coeff = lax.fori_loop(jnp.int32(0), jnp.int32(sections), per_batch, (resid, coeff))
    rms = jnp.sqrt(lax.optimization_barrier(jnp.sum(resid * resid, axis=0)) / resid.shape[0])
    return (resid, coeff, rms)
```

```python
import jax
import jax.numpy as jnp
from jax import lax
from jax.sharding import PartitionSpec as P

TILE = 128


def exchange(blocks, axis):
    return lax.all_to_all(blocks, axis, split_axis=0, concat_axis=0, tiled=True)


def summed(blocks, axis):
    own = exchange(blocks, axis).sum(axis=0)
    return exchange(jnp.broadcast_to(own, blocks.shape), axis)


def shifted(value, axis, steps):
    count = lax.axis_size(axis)
    pairs = [(source, (source + steps) % count) for source in range(count)]
    return lax.ppermute(value, axis, pairs)


def dot(a, b, over):
    return lax.dot_general(
        a, b, ((over[0], over[1]), ((), ())), precision=lax.Precision.HIGH,
        preferred_element_type=jnp.float32,
    )


def upper(basis):
    tiles = basis.shape[1] // TILE
    rows = []
    for i in range(tiles):
        strip = dot(basis[:, i * TILE:(i + 1) * TILE], basis[:, i * TILE:], ((0,), (0,)))
        rows += [strip[:, j * TILE:(j + 1) * TILE] for j in range(tiles - i)]
    return jnp.concatenate(rows, 0)


def whole(packed, tiles):
    part, at = {}, 0
    for i in range(tiles):
        for j in range(i, tiles):
            tile = packed[at * TILE:(at + 1) * TILE]
            part[i, j] = tile
            if i != j:
                part[j, i] = tile.T
            at += 1
    return jnp.concatenate(
        [jnp.concatenate([part[i, j] for j in range(tiles)], 1) for i in range(tiles)], 0
    )


def both(first, gram):
    return 2.0 * first - dot(gram, first, ((1,), (0,)))


def per_device(snapshots, basis):
    sections = lax.axis_size("segment")
    lines = lax.axis_size("row")
    position = lax.axis_index("segment")
    width = snapshots.shape[1]
    size = basis.shape[1]
    tiles = size // TILE
    total_rows = basis.shape[0] * lines
    onward = shifted(basis, "segment", -1)

    first = dot(basis, snapshots, ((0,), (0,)))
    gram = upper(basis)
    share = len(gram) // lines
    sent = jnp.concatenate(
        [gram.reshape(lines, -1, TILE), first.reshape(lines, -1, TILE)], 1
    )
    got = summed(sent, "row")
    got_next = shifted(got, "segment", -1)
    first = got[:, share:].reshape(size, width)
    here = both(first, whole(got[:, :share].reshape(-1, TILE), tiles))
    vec = snapshots - dot(basis, here, ((1,), (0,)))

    first = dot(onward, vec, ((0,), (0,)))
    first = summed(first.reshape(lines, -1, width), "row").reshape(size, width)
    there = both(first, whole(got_next[:, :share].reshape(-1, TILE), tiles))
    vec = vec - dot(onward, there, ((1,), (0,)))

    arrived = shifted(there, "segment", 1)
    squares = jnp.sum(vec * vec, axis=0)
    sums = exchange(jnp.broadcast_to(squares, (lines, width)), "row").sum(axis=0)
    rms = jnp.sqrt(sums / total_rows)
    coeff = jnp.zeros((size, width * sections), jnp.float32)
    coeff = lax.dynamic_update_slice(coeff, here, (jnp.int32(0), position * width))
    before = (position - 1) % sections
    coeff = lax.dynamic_update_slice(coeff, arrived, (jnp.int32(0), before * width))
    return (vec, coeff, rms)


def solution(mesh):
    placed = (P("row", "segment"), P("row", "segment"))
    return jax.shard_map(
        per_device,
        mesh=mesh,
        in_specs=placed,
        out_specs=(P("row", "segment"), P("segment", None), P("segment")),
        check_vma=False,
    )
```

```python
import jax
import jax.numpy as jnp
from jax import lax
from jax.sharding import PartitionSpec as P

TILE = 128


NEAR = 4


def exchange(blocks, axis, groups=None):
    return lax.all_to_all(
        blocks, axis, split_axis=0, concat_axis=0, axis_index_groups=groups, tiled=True
    )


def rings(axis):
    count = lax.axis_size(axis)
    near = [[a + b for b in range(NEAR)] for a in range(0, count, NEAR)]
    far = [[a + b for a in range(0, count, NEAR)] for b in range(NEAR)]
    return near, far


def summed_in_turn(lines, axis):
    near, far = rings(axis)
    blocks = exchange(lines.reshape(len(near[0]), -1, TILE), axis, near)
    blocks = exchange(blocks.sum(axis=0).reshape(len(far[0]), -1, TILE), axis, far)
    own = blocks.sum(axis=0)
    blocks = exchange(jnp.broadcast_to(own, blocks.shape), axis, far).reshape(-1, TILE)
    blocks = exchange(jnp.broadcast_to(blocks, (len(near[0]), *blocks.shape)), axis, near)
    return blocks.reshape(-1, TILE)


def summed(blocks, axis):
    own = exchange(blocks, axis).sum(axis=0)
    return exchange(jnp.broadcast_to(own, blocks.shape), axis)


def shifted(value, axis, steps):
    count = lax.axis_size(axis)
    pairs = [(source, (source + steps) % count) for source in range(count)]
    return lax.ppermute(value, axis, pairs)


def dot(a, b, over):
    return lax.dot_general(
        a, b, ((over[0], over[1]), ((), ())), precision=lax.Precision.HIGH,
        preferred_element_type=jnp.float32,
    )


def upper(basis):
    tiles = basis.shape[1] // TILE
    rows = []
    for i in range(tiles):
        strip = dot(basis[:, i * TILE:(i + 1) * TILE], basis[:, i * TILE:], ((0,), (0,)))
        rows += [strip[:, j * TILE:(j + 1) * TILE] for j in range(tiles - i)]
    return jnp.concatenate(rows, 0)


def whole(packed, tiles):
    part, at = {}, 0
    for i in range(tiles):
        for j in range(i, tiles):
            tile = packed[at * TILE:(at + 1) * TILE]
            part[i, j] = tile
            if i != j:
                part[j, i] = tile.T
            at += 1
    return jnp.concatenate(
        [jnp.concatenate([part[i, j] for j in range(tiles)], 1) for i in range(tiles)], 0
    )


def both(first, gram):
    return 2.0 * first - dot(gram, first, ((1,), (0,)))


def per_device(snapshots, basis):
    sections = lax.axis_size("segment")
    lines = lax.axis_size("row")
    position = lax.axis_index("segment")
    width = snapshots.shape[1]
    size = basis.shape[1]
    tiles = size // TILE
    total_rows = basis.shape[0] * lines
    onward = shifted(basis, "segment", -1)

    first = dot(basis, snapshots, ((0,), (0,)))
    gram = upper(basis)
    share = len(gram)
    got = summed_in_turn(jnp.concatenate([gram, first], 0), "row")
    got_next = shifted(got[:share], "segment", -1)
    first = got[share:]
    here = both(first, whole(got[:share], tiles))
    vec = snapshots - dot(basis, here, ((1,), (0,)))

    first = dot(onward, vec, ((0,), (0,)))
    first = summed(first.reshape(lines, -1, width), "row").reshape(size, width)
    there = both(first, whole(got_next, tiles))
    vec = vec - dot(onward, there, ((1,), (0,)))

    arrived = shifted(there, "segment", 1)
    squares = jnp.sum(vec * vec, axis=0)
    sums = exchange(jnp.broadcast_to(squares, (lines, width)), "row").sum(axis=0)
    rms = jnp.sqrt(sums / total_rows)
    coeff = jnp.zeros((size, width * sections), jnp.float32)
    coeff = lax.dynamic_update_slice(coeff, here, (jnp.int32(0), position * width))
    before = (position - 1) % sections
    coeff = lax.dynamic_update_slice(coeff, arrived, (jnp.int32(0), before * width))
    return (vec, coeff, rms)


def solution(mesh):
    placed = (P("row", "segment"), P("row", "segment"))
    return jax.shard_map(
        per_device,
        mesh=mesh,
        in_specs=placed,
        out_specs=(P("row", "segment"), P("segment", None), P("segment")),
        check_vma=False,
    )
```

```python
import jax
import jax.numpy as jnp
from jax import lax
from jax.experimental import pallas as pl
from jax.experimental.pallas import tpu as pltpu
from jax.sharding import PartitionSpec as P

TILE = 128
NEAR = 4


def exchange(blocks, axis, groups=None):
    return lax.all_to_all(
        blocks, axis, split_axis=0, concat_axis=0, axis_index_groups=groups, tiled=True
    )


def rings(axis):
    count = lax.axis_size(axis)
    near = [[a + b for b in range(NEAR)] for a in range(0, count, NEAR)]
    far = [[a + b for a in range(0, count, NEAR)] for b in range(NEAR)]
    return near, far


def summed_in_turn(lines, axis):
    near, far = rings(axis)
    blocks = exchange(lines.reshape(len(near[0]), -1, TILE), axis, near)
    blocks = exchange(blocks.sum(axis=0).reshape(len(far[0]), -1, TILE), axis, far)
    own = blocks.sum(axis=0)
    blocks = exchange(jnp.broadcast_to(own, blocks.shape), axis, far).reshape(-1, TILE)
    blocks = exchange(jnp.broadcast_to(blocks, (len(near[0]), *blocks.shape)), axis, near)
    return blocks.reshape(-1, TILE)


def summed(lines, axis):
    blocks = lines.reshape(lax.axis_size(axis), -1, TILE)
    own = exchange(blocks, axis).sum(axis=0)
    return exchange(jnp.broadcast_to(own, blocks.shape), axis).reshape(-1, TILE)


def shifted(value, axis, steps):
    count = lax.axis_size(axis)
    pairs = [(source, (source + steps) % count) for source in range(count)]
    return lax.ppermute(value, axis, pairs)


def halves(value):
    high = value.astype(jnp.bfloat16)
    return high, (value - high.astype(jnp.float32)).astype(jnp.bfloat16)


def product(a, b):
    def once(x, y):
        return jnp.dot(x, y, preferred_element_type=jnp.float32)

    return once(a[0], b[0]) + (once(a[0], b[1]) + once(a[1], b[0]))


def tiles_of(size):
    count = size // TILE
    return [(i, j) for i in range(count) for j in range(i, count)]


def start_kernel(basis_ref, vec_ref, out_ref):
    basis = basis_ref[...]
    size = basis.shape[1]
    count = size // TILE
    turned = halves(basis.T)
    right = halves(jnp.concatenate([basis, vec_ref[...]], axis=1))
    at = 0
    for i in range(count):
        left = tuple(part[i * TILE:(i + 1) * TILE] for part in turned)
        strip = product(left, tuple(part[:, i * TILE:] for part in right))
        for j in range(count - i):
            out_ref[at:at + TILE] = strip[:, j * TILE:(j + 1) * TILE]
            at += TILE
        base = (len(tiles_of(size)) + i) * TILE
        out_ref[base:base + TILE] = strip[:, (count - i) * TILE:]


def both(first, gram_ref, size):
    count = size // TILE
    part = {}
    for at, (i, j) in enumerate(tiles_of(size)):
        tile = gram_ref[at * TILE:(at + 1) * TILE]
        part[i, j] = tile
        if i != j:
            part[j, i] = tile.T
    right = halves(first)
    rows = []
    for i in range(count):
        row = jnp.concatenate([part[i, j] for j in range(count)], axis=1)
        rows.append(product(halves(row), right))
    return 2.0 * first - jnp.concatenate(rows, axis=0)


def turn_kernel(got_ref, basis_ref, vec_ref, next_ref, here_ref, vec_out, first_out):
    size = basis_ref.shape[1]
    here = both(got_ref[got_ref.shape[0] - size:], got_ref, size)
    here_ref[...] = here
    vec = vec_ref[...] - product(halves(basis_ref[...]), halves(here))
    vec_out[...] = vec
    first_out[...] = product(halves(next_ref[...].T), halves(vec))


def end_kernel(first_ref, gram_ref, basis_ref, vec_ref, there_ref, vec_out, squares_ref):
    there = both(first_ref[...], gram_ref, basis_ref.shape[1])
    there_ref[...] = there
    vec = vec_ref[...] - product(halves(basis_ref[...]), halves(there))
    vec_out[...] = vec
    squares_ref[...] = jnp.sum(vec * vec, axis=0, keepdims=True)


def local(kernel, ins, *shapes):
    outs = [jax.ShapeDtypeStruct(shape, jnp.float32) for shape in shapes]
    return pl.pallas_call(
        kernel,
        in_specs=[pl.BlockSpec(memory_space=pltpu.VMEM)] * ins,
        out_specs=[pl.BlockSpec(memory_space=pltpu.VMEM)] * len(outs),
        out_shape=outs,
        compiler_params=pltpu.CompilerParams(vmem_limit_bytes=16 * 2**20),
    )


def per_device(snapshots, basis):
    sections = lax.axis_size("segment")
    lines = lax.axis_size("row")
    position = lax.axis_index("segment")
    rows, width = snapshots.shape
    size = basis.shape[1]
    share = len(tiles_of(size)) * TILE
    total_rows = rows * lines
    onward = shifted(basis, "segment", -1)

    sent = local(start_kernel, 2, (share + size, TILE))(basis, snapshots)[0]
    got = summed_in_turn(sent, "row")
    gram_next = shifted(got[:share], "segment", -1)
    here, vec, first = local(turn_kernel, 4, (size, width), (rows, width), (size, width))(
        got, basis, snapshots, onward
    )
    first = summed(first, "row")
    there, vec, squares = local(end_kernel, 4, (size, width), (rows, width), (1, width))(
        first, gram_next, onward, vec
    )

    arrived = shifted(there, "segment", 1)
    sums = exchange(jnp.broadcast_to(squares, (lines, width)), "row").sum(axis=0)
    rms = jnp.sqrt(sums / total_rows)
    coeff = jnp.zeros((size, width * sections), jnp.float32)
    coeff = lax.dynamic_update_slice(coeff, here, (jnp.int32(0), position * width))
    before = (position - 1) % sections
    coeff = lax.dynamic_update_slice(coeff, arrived, (jnp.int32(0), before * width))
    return (vec, coeff, rms)


def solution(mesh):
    placed = (P("row", "segment"), P("row", "segment"))
    return jax.shard_map(
        per_device,
        mesh=mesh,
        in_specs=placed,
        out_specs=(P("row", "segment"), P("segment", None), P("segment")),
        check_vma=False,
    )
```

```python
import jax
import jax.numpy as jnp
from jax import lax
from jax.experimental import pallas as pl
from jax.experimental.pallas import tpu as pltpu
from jax.sharding import PartitionSpec as P


TILE = 128
NEAR = 4


def exchange(blocks, axis, groups=None):
    return lax.all_to_all(
        blocks, axis, split_axis=0, concat_axis=0, axis_index_groups=groups, tiled=True
    )


def rings(axis):
    count = lax.axis_size(axis)
    near = [[a + b for b in range(NEAR)] for a in range(0, count, NEAR)]
    far = [[a + b for a in range(0, count, NEAR)] for b in range(NEAR)]
    return near, far


def gathered(mine, near, far):
    blocks = exchange(mine.reshape(len(far[0]), -1, TILE), "row", far)
    own = blocks.sum(axis=0)
    blocks = exchange(jnp.broadcast_to(own, blocks.shape), "row", far).reshape(-1, TILE)
    blocks = exchange(jnp.broadcast_to(blocks, (len(near[0]), *blocks.shape)), "row", near)
    return blocks.reshape(-1, TILE)


def shifted(value, axis, steps):
    count = lax.axis_size(axis)
    pairs = [(source, (source + steps) % count) for source in range(count)]
    return lax.ppermute(value, axis, pairs)


def halves(value):
    high = value.astype(jnp.bfloat16)
    return high, (value - high.astype(jnp.float32)).astype(jnp.bfloat16)


def product(a, b):
    def once(x, y):
        return jnp.dot(x, y, preferred_element_type=jnp.float32)

    return once(a[0], b[0]) + (once(a[0], b[1]) + once(a[1], b[0]))


def tiles_of(size):
    count = size // TILE
    return [(i, j) for i in range(count) for j in range(i, count)]


def start_kernel(basis_hbm, vec_hbm, out_ref, basis_ref, vec_ref, done):
    copies = [
        pltpu.make_async_copy(basis_hbm, basis_ref, done.at[0]),
        pltpu.make_async_copy(vec_hbm, vec_ref, done.at[1]),
    ]
    for copy in copies:
        copy.start()
    for copy in copies:
        copy.wait()
    basis = basis_ref[...]
    size = basis.shape[1]
    count = size // TILE
    turned = halves(basis.T)
    right = halves(jnp.concatenate([basis, vec_ref[...]], axis=1))
    at = 0
    for i in range(count):
        left = tuple(part[i * TILE:(i + 1) * TILE] for part in turned)
        strip = product(left, tuple(part[:, i * TILE:] for part in right))
        for j in range(count - i):
            out_ref[at:at + TILE] = strip[:, j * TILE:(j + 1) * TILE]
            at += TILE
        base = (len(tiles_of(size)) + i) * TILE
        out_ref[base:base + TILE] = strip[:, (count - i) * TILE:]


def both(first, gram_ref, size):
    count = size // TILE
    part = {}
    for at, (i, j) in enumerate(tiles_of(size)):
        tile = gram_ref[at * TILE:(at + 1) * TILE]
        part[i, j] = tile
        if i != j:
            part[j, i] = tile.T
    right = halves(first)
    rows = []
    for i in range(count):
        row = jnp.concatenate([part[i, j] for j in range(count)], axis=1)
        rows.append(product(halves(row), right))
    return 2.0 * first - jnp.concatenate(rows, axis=0)


def turn_kernel(
    got_ref, basis_ref, vec_ref, next_ref, vec_out, first_out, coeff_hbm, here_ref, zero_ref, done
):
    size = basis_ref.shape[1]
    width = vec_ref.shape[1]
    sections = coeff_hbm.shape[1] // width
    zero_ref[...] = jnp.zeros_like(zero_ref)
    fills = [
        pltpu.make_async_copy(
            zero_ref, coeff_hbm.at[:, b * width:(b + 1) * width], done.at[b]
        )
        for b in range(sections)
    ]
    for fill in fills:
        fill.start()
    here = both(got_ref[got_ref.shape[0] - size:], got_ref, size)
    here_ref[...] = here
    vec = vec_ref[...] - product(halves(basis_ref[...]), halves(here))
    vec_out[...] = vec
    for fill in fills:
        fill.wait()
    column = pl.multiple_of(lax.axis_index("segment") * width, width)
    own = pltpu.make_async_copy(
        here_ref, coeff_hbm.at[:, pl.ds(column, width)], done.at[sections]
    )
    own.start()
    first_out[...] = product(halves(next_ref[...].T), halves(vec))
    own.wait()


def end_kernel(first_ref, gram_ref, basis_ref, vec_ref, there_ref, vec_out, squares_ref):
    there = both(first_ref[...], gram_ref, basis_ref.shape[1])
    there_ref[...] = there
    vec = vec_ref[...] - product(halves(basis_ref[...]), halves(there))
    vec_out[...] = vec
    squares_ref[...] = jnp.sum(vec * vec, axis=0, keepdims=True)


def local(kernel, ins, outs, scratch=()):
    return pl.pallas_call(
        kernel,
        in_specs=[pl.BlockSpec(memory_space=space) for space in ins],
        out_specs=[pl.BlockSpec(memory_space=space) for space, _ in outs],
        out_shape=[jax.ShapeDtypeStruct(shape, jnp.float32) for _, shape in outs],
        scratch_shapes=scratch,
        compiler_params=pltpu.CompilerParams(vmem_limit_bytes=16 * 2**20),
    )


def per_device(snapshots, basis):
    sections = lax.axis_size("segment")
    lines = lax.axis_size("row")
    position = lax.axis_index("segment")
    rows, width = snapshots.shape
    size = basis.shape[1]
    share = len(tiles_of(size)) * TILE
    total_rows = rows * lines
    hbm = pltpu.HBM
    near, far = rings("row")

    onward = shifted(basis, "segment", -1)
    (sent,) = local(
        start_kernel, (hbm, hbm), [(pltpu.VMEM, (share + size, TILE))],
        (pltpu.VMEM(basis.shape, jnp.float32), pltpu.VMEM(snapshots.shape, jnp.float32),
         pltpu.SemaphoreType.DMA((2,))),
    )(*(pltpu.with_memory_space_constraint(array, hbm) for array in (basis, snapshots)))
    blocks = exchange(sent.reshape(len(near[0]), -1, TILE), "row", near)
    mine, onward = lax.optimization_barrier((blocks.sum(axis=0), onward))
    got = gathered(mine, near, far)
    gram_next = shifted(got, "segment", -1)
    vec, first, coeff = local(
        turn_kernel, (pltpu.VMEM,) * 4,
        [(pltpu.VMEM, (rows, width)), (pltpu.VMEM, (size, width)),
         (hbm, (size, width * sections))],
        (pltpu.VMEM((size, width), jnp.float32), pltpu.VMEM((size, width), jnp.float32),
         pltpu.SemaphoreType.DMA((sections + 1,))),
    )(got, basis, snapshots, onward)
    blocks = exchange(first.reshape(lines, -1, TILE), "row")
    blocks, gram_next = lax.optimization_barrier((blocks, gram_next))
    first = exchange(jnp.broadcast_to(blocks.sum(axis=0), blocks.shape), "row")
    there, vec, squares = local(
        end_kernel, (pltpu.VMEM,) * 4,
        [(pltpu.VMEM, (size, width)), (pltpu.VMEM, (rows, width)), (pltpu.VMEM, (1, width))],
    )(first.reshape(-1, TILE), gram_next, onward, vec)

    arrived = shifted(there, "segment", 1)
    blocks = exchange(jnp.broadcast_to(squares, (lines, width)), "row")
    before = (position - 1) % sections
    coeff = lax.dynamic_update_slice(coeff, arrived, (jnp.int32(0), before * width))
    blocks, coeff = lax.optimization_barrier((blocks, coeff))
    rms = jnp.sqrt(blocks.sum(axis=0) / total_rows)
    return (vec, coeff, rms)


def solution(mesh):
    placed = (P("row", "segment"), P("row", "segment"))
    return jax.shard_map(
        per_device,
        mesh=mesh,
        in_specs=placed,
        out_specs=(P("row", "segment"), P("segment", None), P("segment")),
        check_vma=False,
    )
```

```python
import jax
import jax.numpy as jnp
from jax import lax
from jax.experimental import pallas as pl
from jax.experimental.pallas import tpu as pltpu
from jax.sharding import PartitionSpec as P


TILE = 128
NEAR = 4


def exchange(blocks, axis, groups=None):
    return lax.all_to_all(
        blocks, axis, split_axis=0, concat_axis=0, axis_index_groups=groups, tiled=True
    )


def rings(axis):
    count = lax.axis_size(axis)
    near = [[a + b for b in range(NEAR)] for a in range(0, count, NEAR)]
    far = [[a + b for a in range(0, count, NEAR)] for b in range(NEAR)]
    return near, far


def gathered(mine, near, far):
    blocks = exchange(mine.reshape(len(far[0]), -1, TILE), "row", far)
    own = blocks.sum(axis=0)
    blocks = exchange(jnp.broadcast_to(own, blocks.shape), "row", far).reshape(-1, TILE)
    blocks = exchange(jnp.broadcast_to(blocks, (len(near[0]), *blocks.shape)), "row", near)
    return blocks.reshape(-1, TILE)


def shifted(value, axis, steps):
    count = lax.axis_size(axis)
    pairs = [(source, (source + steps) % count) for source in range(count)]
    return lax.ppermute(value, axis, pairs)


def halves(value):
    high = value.astype(jnp.bfloat16)
    return high, (value - high.astype(jnp.float32)).astype(jnp.bfloat16)


def product(a, b):
    def once(x, y):
        return jnp.dot(x, y, preferred_element_type=jnp.float32)

    return once(a[0], b[0]) + (once(a[0], b[1]) + once(a[1], b[0]))


def tiles_of(size):
    count = size // TILE
    return [(i, j) for i in range(count) for j in range(i, count)]


def start_kernel(basis_hbm, vec_hbm, out_ref, basis_ref, vec_ref, done):
    copies = [
        pltpu.make_async_copy(basis_hbm, basis_ref, done.at[0]),
        pltpu.make_async_copy(vec_hbm, vec_ref, done.at[1]),
    ]
    for copy in copies:
        copy.start()
    for copy in copies:
        copy.wait()
    basis = basis_ref[...]
    size = basis.shape[1]
    count = size // TILE
    turned = halves(basis.T)
    right = halves(jnp.concatenate([basis, vec_ref[...]], axis=1))
    at = 0
    for i in range(count):
        left = tuple(part[i * TILE:(i + 1) * TILE] for part in turned)
        strip = product(left, tuple(part[:, i * TILE:] for part in right))
        for j in range(count - i):
            out_ref[at:at + TILE] = strip[:, j * TILE:(j + 1) * TILE]
            at += TILE
        base = (len(tiles_of(size)) + i) * TILE
        out_ref[base:base + TILE] = strip[:, (count - i) * TILE:]


def both(first, gram_ref, size):
    count = size // TILE
    part = {}
    for at, (i, j) in enumerate(tiles_of(size)):
        tile = gram_ref[at * TILE:(at + 1) * TILE]
        part[i, j] = tile
        if i != j:
            part[j, i] = tile.T
    right = halves(first)
    rows = []
    for i in range(count):
        row = jnp.concatenate([part[i, j] for j in range(count)], axis=1)
        rows.append(product(halves(row), right))
    return 2.0 * first - jnp.concatenate(rows, axis=0)


def turn_kernel(
    got_ref, basis_ref, vec_ref, next_ref, here_ref, vec_out, first_out, coeff_hbm, zero_ref, done
):
    size = basis_ref.shape[1]
    width = vec_ref.shape[1]
    zero_ref[...] = jnp.zeros_like(zero_ref)
    fills = [
        pltpu.make_async_copy(
            zero_ref, coeff_hbm.at[:, b * width:(b + 1) * width], done.at[b]
        )
        for b in range(coeff_hbm.shape[1] // width)
    ]
    for fill in fills:
        fill.start()
    here = both(got_ref[got_ref.shape[0] - size:], got_ref, size)
    here_ref[...] = here
    vec = vec_ref[...] - product(halves(basis_ref[...]), halves(here))
    vec_out[...] = vec
    first_out[...] = product(halves(next_ref[...].T), halves(vec))
    for fill in fills:
        fill.wait()


def end_kernel(first_ref, gram_ref, basis_ref, vec_ref, there_ref, vec_out, squares_ref):
    there = both(first_ref[...], gram_ref, basis_ref.shape[1])
    there_ref[...] = there
    vec = vec_ref[...] - product(halves(basis_ref[...]), halves(there))
    vec_out[...] = vec
    squares_ref[...] = jnp.sum(vec * vec, axis=0, keepdims=True)


def local(kernel, ins, outs, scratch=()):
    return pl.pallas_call(
        kernel,
        in_specs=[pl.BlockSpec(memory_space=space) for space in ins],
        out_specs=[pl.BlockSpec(memory_space=space) for space, _ in outs],
        out_shape=[jax.ShapeDtypeStruct(shape, jnp.float32) for _, shape in outs],
        scratch_shapes=scratch,
        compiler_params=pltpu.CompilerParams(vmem_limit_bytes=16 * 2**20),
    )


def per_device(snapshots, basis):
    sections = lax.axis_size("segment")
    lines = lax.axis_size("row")
    position = lax.axis_index("segment")
    rows, width = snapshots.shape
    size = basis.shape[1]
    share = len(tiles_of(size)) * TILE
    total_rows = rows * lines
    hbm = pltpu.HBM
    near, far = rings("row")

    onward = shifted(basis, "segment", -1)
    (sent,) = local(
        start_kernel, (hbm, hbm), [(pltpu.VMEM, (share + size, TILE))],
        (pltpu.VMEM(basis.shape, jnp.float32), pltpu.VMEM(snapshots.shape, jnp.float32),
         pltpu.SemaphoreType.DMA((2,))),
    )(*(pltpu.with_memory_space_constraint(array, hbm) for array in (basis, snapshots)))
    blocks = exchange(sent.reshape(len(near[0]), -1, TILE), "row", near)
    mine, onward = lax.optimization_barrier((blocks.sum(axis=0), onward))
    got = gathered(mine, near, far)
    gram_next = shifted(got[:share], "segment", -1)
    here, vec, first, coeff = local(
        turn_kernel, (pltpu.VMEM,) * 4,
        [(pltpu.VMEM, (size, width)), (pltpu.VMEM, (rows, width)),
         (pltpu.VMEM, (size, width)), (hbm, (size, width * sections))],
        (pltpu.VMEM((size, width), jnp.float32), pltpu.SemaphoreType.DMA((sections,))),
    )(got, basis, snapshots, onward)
    blocks = exchange(first.reshape(lines, -1, TILE), "row")
    mine, gram_next = lax.optimization_barrier((blocks.sum(axis=0), gram_next))
    first = exchange(jnp.broadcast_to(mine, blocks.shape), "row")
    there, vec, squares = local(
        end_kernel, (pltpu.VMEM,) * 4,
        [(pltpu.VMEM, (size, width)), (pltpu.VMEM, (rows, width)), (pltpu.VMEM, (1, width))],
    )(first.reshape(-1, TILE), gram_next, onward, vec)

    arrived = shifted(there, "segment", 1)
    blocks = exchange(jnp.broadcast_to(squares, (lines, width)), "row")
    coeff = lax.dynamic_update_slice(coeff, here, (jnp.int32(0), position * width))
    before = (position - 1) % sections
    coeff = lax.dynamic_update_slice(coeff, arrived, (jnp.int32(0), before * width))
    blocks, coeff = lax.optimization_barrier((blocks, coeff))
    rms = jnp.sqrt(blocks.sum(axis=0) / total_rows)
    return (vec, coeff, rms)


def solution(mesh):
    placed = (P("row", "segment"), P("row", "segment"))
    return jax.shard_map(
        per_device,
        mesh=mesh,
        in_specs=placed,
        out_specs=(P("row", "segment"), P("segment", None), P("segment")),
        check_vma=False,
    )
```

```python
import jax
import jax.numpy as jnp
from jax import lax
from jax.experimental import pallas as pl
from jax.experimental.pallas import tpu as pltpu
from jax.sharding import PartitionSpec as P


TILE = 128
NEAR = 4


def exchange(blocks, axis, groups=None):
    return lax.all_to_all(
        blocks, axis, split_axis=0, concat_axis=0, axis_index_groups=groups, tiled=True
    )


def rings(axis):
    count = lax.axis_size(axis)
    near = [[a + b for b in range(NEAR)] for a in range(0, count, NEAR)]
    far = [[a + b for a in range(0, count, NEAR)] for b in range(NEAR)]
    return near, far


def gathered(mine, near, far):
    blocks = exchange(mine.reshape(len(far[0]), -1, TILE), "row", far)
    own = blocks.sum(axis=0)
    blocks = exchange(jnp.broadcast_to(own, blocks.shape), "row", far).reshape(-1, TILE)
    blocks = exchange(jnp.broadcast_to(blocks, (len(near[0]), *blocks.shape)), "row", near)
    return blocks.reshape(-1, TILE)


def shifted(value, axis, steps):
    count = lax.axis_size(axis)
    pairs = [(source, (source + steps) % count) for source in range(count)]
    return lax.ppermute(value, axis, pairs)


def halves(value):
    high = value.astype(jnp.bfloat16)
    return high, (value - high.astype(jnp.float32)).astype(jnp.bfloat16)


def product(a, b):
    def once(x, y):
        return jnp.dot(x, y, preferred_element_type=jnp.float32)

    return once(a[0], b[0]) + (once(a[0], b[1]) + once(a[1], b[0]))


def tiles_of(size):
    count = size // TILE
    return [(i, j) for i in range(count) for j in range(i, count)]


def start_kernel(basis_hbm, vec_hbm, out_ref, basis_ref, vec_ref, done):
    copies = [
        pltpu.make_async_copy(basis_hbm, basis_ref, done.at[0]),
        pltpu.make_async_copy(vec_hbm, vec_ref, done.at[1]),
    ]
    for copy in copies:
        copy.start()
    for copy in copies:
        copy.wait()
    basis = basis_ref[...]
    size = basis.shape[1]
    count = size // TILE
    turned = halves(basis.T)
    right = halves(jnp.concatenate([basis, vec_ref[...]], axis=1))
    at = 0
    for i in range(count):
        left = tuple(part[i * TILE:(i + 1) * TILE] for part in turned)
        strip = product(left, tuple(part[:, i * TILE:] for part in right))
        for j in range(count - i):
            out_ref[at:at + TILE] = strip[:, j * TILE:(j + 1) * TILE]
            at += TILE
        base = (len(tiles_of(size)) + i) * TILE
        out_ref[base:base + TILE] = strip[:, (count - i) * TILE:]


def both(first, gram_ref, size):
    count = size // TILE
    part = {}
    for at, (i, j) in enumerate(tiles_of(size)):
        tile = gram_ref[at * TILE:(at + 1) * TILE]
        part[i, j] = tile
        if i != j:
            part[j, i] = tile.T
    right = halves(first)
    rows = []
    for i in range(count):
        row = jnp.concatenate([part[i, j] for j in range(count)], axis=1)
        rows.append(product(halves(row), right))
    return 2.0 * first - jnp.concatenate(rows, axis=0)


def turn_kernel(got_ref, basis_ref, vec_ref, next_ref, here_ref, vec_out, first_out):
    size = basis_ref.shape[1]
    here = both(got_ref[got_ref.shape[0] - size:], got_ref, size)
    here_ref[...] = here
    vec = vec_ref[...] - product(halves(basis_ref[...]), halves(here))
    vec_out[...] = vec
    first_out[...] = product(halves(next_ref[...].T), halves(vec))


def end_kernel(first_ref, gram_ref, basis_ref, vec_ref, there_ref, vec_out, squares_ref):
    there = both(first_ref[...], gram_ref, basis_ref.shape[1])
    there_ref[...] = there
    vec = vec_ref[...] - product(halves(basis_ref[...]), halves(there))
    vec_out[...] = vec
    squares_ref[...] = jnp.sum(vec * vec, axis=0, keepdims=True)


def local(kernel, ins, outs, scratch=()):
    return pl.pallas_call(
        kernel,
        in_specs=[pl.BlockSpec(memory_space=space) for space in ins],
        out_specs=[pl.BlockSpec(memory_space=space) for space, _ in outs],
        out_shape=[jax.ShapeDtypeStruct(shape, jnp.float32) for _, shape in outs],
        scratch_shapes=scratch,
        compiler_params=pltpu.CompilerParams(vmem_limit_bytes=16 * 2**20),
    )


def per_device(snapshots, basis):
    sections = lax.axis_size("segment")
    lines = lax.axis_size("row")
    position = lax.axis_index("segment")
    rows, width = snapshots.shape
    size = basis.shape[1]
    share = len(tiles_of(size)) * TILE
    total_rows = rows * lines
    hbm = pltpu.HBM
    near, far = rings("row")

    onward = shifted(basis, "segment", -1)
    (sent,) = local(
        start_kernel, (hbm, hbm), [(pltpu.VMEM, (share + size, TILE))],
        (pltpu.VMEM(basis.shape, jnp.float32), pltpu.VMEM(snapshots.shape, jnp.float32),
         pltpu.SemaphoreType.DMA((2,))),
    )(*(pltpu.with_memory_space_constraint(array, hbm) for array in (basis, snapshots)))
    blocks = exchange(sent.reshape(len(near[0]), -1, TILE), "row", near)
    mine, onward = lax.optimization_barrier((blocks.sum(axis=0), onward))
    got = gathered(mine, near, far)
    gram_next = shifted(got[:share], "segment", -1)
    here, vec, first = local(
        turn_kernel, (pltpu.VMEM,) * 4,
        [(pltpu.VMEM, (size, width)), (pltpu.VMEM, (rows, width)), (pltpu.VMEM, (size, width))],
    )(got, basis, snapshots, onward)
    coeff = jnp.zeros((size, width * sections), jnp.float32)
    coeff = lax.dynamic_update_slice(coeff, here, (jnp.int32(0), position * width))
    blocks = exchange(first.reshape(lines, -1, TILE), "row")
    mine, coeff = lax.optimization_barrier((blocks.sum(axis=0), coeff))
    first = exchange(jnp.broadcast_to(mine, blocks.shape), "row")
    first, gram_next = lax.optimization_barrier((first, gram_next))
    there, vec, squares = local(
        end_kernel, (pltpu.VMEM,) * 4,
        [(pltpu.VMEM, (size, width)), (pltpu.VMEM, (rows, width)), (pltpu.VMEM, (1, width))],
    )(first.reshape(-1, TILE), gram_next, onward, vec)

    arrived = shifted(there, "segment", 1)
    blocks = exchange(jnp.broadcast_to(squares, (lines, width)), "row")
    before = (position - 1) % sections
    coeff = lax.dynamic_update_slice(coeff, arrived, (jnp.int32(0), before * width))
    blocks, coeff = lax.optimization_barrier((blocks, coeff))
    rms = jnp.sqrt(blocks.sum(axis=0) / total_rows)
    return (vec, coeff, rms)


def solution(mesh):
    placed = (P("row", "segment"), P("row", "segment"))
    return jax.shard_map(
        per_device,
        mesh=mesh,
        in_specs=placed,
        out_specs=(P("row", "segment"), P("segment", None), P("segment")),
        check_vma=False,
    )
```

```python
import jax
import jax.numpy as jnp
from jax import lax
from jax.experimental import pallas as pl
from jax.experimental.pallas import tpu as pltpu
from jax.sharding import PartitionSpec as P


TILE = 128
NEAR = 4


def exchange(blocks, axis, groups=None):
    return lax.all_to_all(
        blocks, axis, split_axis=0, concat_axis=0, axis_index_groups=groups, tiled=True
    )


def rings(axis):
    count = lax.axis_size(axis)
    near = [[a + b for b in range(NEAR)] for a in range(0, count, NEAR)]
    far = [[a + b for a in range(0, count, NEAR)] for b in range(NEAR)]
    return near, far


def gathered(mine, near, far):
    blocks = exchange(mine.reshape(len(far[0]), -1, TILE), "row", far)
    own = blocks.sum(axis=0)
    blocks = exchange(jnp.broadcast_to(own, blocks.shape), "row", far).reshape(-1, TILE)
    blocks = exchange(jnp.broadcast_to(blocks, (len(near[0]), *blocks.shape)), "row", near)
    return blocks.reshape(-1, TILE)


def shifted(value, axis, steps):
    count = lax.axis_size(axis)
    pairs = [(source, (source + steps) % count) for source in range(count)]
    return lax.ppermute(value, axis, pairs)


def halves(value):
    high = value.astype(jnp.bfloat16)
    return high, (value - high.astype(jnp.float32)).astype(jnp.bfloat16)


def product(a, b):
    def once(x, y):
        return jnp.dot(x, y, preferred_element_type=jnp.float32)

    return once(a[0], b[0]) + (once(a[0], b[1]) + once(a[1], b[0]))


def tiles_of(size):
    count = size // TILE
    return [(i, j) for i in range(count) for j in range(i, count)]


def start_kernel(basis_hbm, vec_hbm, out_ref, basis_ref, vec_ref, done):
    copies = [
        pltpu.make_async_copy(basis_hbm, basis_ref, done.at[0]),
        pltpu.make_async_copy(vec_hbm, vec_ref, done.at[1]),
    ]
    for copy in copies:
        copy.start()
    for copy in copies:
        copy.wait()
    basis = basis_ref[...]
    size = basis.shape[1]
    count = size // TILE
    turned = halves(basis.T)
    right = halves(jnp.concatenate([basis, vec_ref[...]], axis=1))
    at = 0
    for i in range(count):
        left = tuple(part[i * TILE:(i + 1) * TILE] for part in turned)
        strip = product(left, tuple(part[:, i * TILE:] for part in right))
        for j in range(count - i):
            out_ref[at:at + TILE] = strip[:, j * TILE:(j + 1) * TILE]
            at += TILE
        base = (len(tiles_of(size)) + i) * TILE
        out_ref[base:base + TILE] = strip[:, (count - i) * TILE:]


def both(first, gram_ref, size):
    count = size // TILE
    part = {}
    for at, (i, j) in enumerate(tiles_of(size)):
        tile = gram_ref[at * TILE:(at + 1) * TILE]
        part[i, j] = tile
        if i != j:
            part[j, i] = tile.T
    right = halves(first)
    rows = []
    for i in range(count):
        row = jnp.concatenate([part[i, j] for j in range(count)], axis=1)
        rows.append(product(halves(row), right))
    return 2.0 * first - jnp.concatenate(rows, axis=0)


def turn_kernel(got_ref, basis_ref, vec_ref, next_ref, here_ref, vec_out, first_out):
    size = basis_ref.shape[1]
    here = both(got_ref[got_ref.shape[0] - size:], got_ref, size)
    here_ref[...] = here
    vec = vec_ref[...] - product(halves(basis_ref[...]), halves(here))
    vec_out[...] = vec
    first_out[...] = product(halves(next_ref[...].T), halves(vec))


def end_kernel(first_ref, gram_ref, basis_ref, vec_ref, there_ref, vec_out, squares_ref):
    there = both(first_ref[...], gram_ref, basis_ref.shape[1])
    there_ref[...] = there
    vec = vec_ref[...] - product(halves(basis_ref[...]), halves(there))
    vec_out[...] = vec
    squares = jnp.sum(vec * vec, axis=0, keepdims=True)
    squares_ref[...] = jnp.broadcast_to(squares[None], squares_ref.shape)


def local(kernel, ins, outs, scratch=()):
    return pl.pallas_call(
        kernel,
        in_specs=[pl.BlockSpec(memory_space=space) for space in ins],
        out_specs=[pl.BlockSpec(memory_space=space) for space, _ in outs],
        out_shape=[jax.ShapeDtypeStruct(shape, jnp.float32) for _, shape in outs],
        scratch_shapes=scratch,
        compiler_params=pltpu.CompilerParams(vmem_limit_bytes=16 * 2**20),
    )


def per_device(snapshots, basis):
    sections = lax.axis_size("segment")
    lines = lax.axis_size("row")
    position = lax.axis_index("segment")
    rows, width = snapshots.shape
    size = basis.shape[1]
    share = len(tiles_of(size)) * TILE
    total_rows = rows * lines
    hbm = pltpu.HBM
    near, far = rings("row")

    onward = shifted(basis, "segment", -1)
    (sent,) = local(
        start_kernel, (hbm, hbm), [(pltpu.VMEM, (share + size, TILE))],
        (pltpu.VMEM(basis.shape, jnp.float32), pltpu.VMEM(snapshots.shape, jnp.float32),
         pltpu.SemaphoreType.DMA((2,))),
    )(*(pltpu.with_memory_space_constraint(array, hbm) for array in (basis, snapshots)))
    blocks = exchange(sent.reshape(len(near[0]), -1, TILE), "row", near)
    mine, onward = lax.optimization_barrier((blocks.sum(axis=0), onward))
    got = gathered(mine, near, far)
    gram_next = shifted(got[:share], "segment", -1)
    here, vec, first = local(
        turn_kernel, (pltpu.VMEM,) * 4,
        [(pltpu.VMEM, (size, width)), (pltpu.VMEM, (rows, width)), (pltpu.VMEM, (size, width))],
    )(got, basis, snapshots, onward)
    coeff = jnp.zeros((size, width * sections), jnp.float32)
    coeff = lax.dynamic_update_slice(coeff, here, (jnp.int32(0), position * width))
    blocks = exchange(first.reshape(lines, -1, TILE), "row")
    mine, coeff = lax.optimization_barrier((blocks.sum(axis=0), coeff))
    first = exchange(jnp.broadcast_to(mine, blocks.shape), "row")
    first = lax.optimization_barrier(first)
    first, gram_next = lax.optimization_barrier((first, gram_next))
    there, vec, squares = local(
        end_kernel, (pltpu.VMEM,) * 4,
        [(pltpu.VMEM, (size, width)), (pltpu.VMEM, (rows, width)),
         (pltpu.VMEM, (lines, 1, width))],
    )(first.reshape(-1, TILE), gram_next, onward, vec)

    arrived = shifted(there, "segment", 1)
    blocks = exchange(squares, "row")
    before = (position - 1) % sections
    coeff = lax.dynamic_update_slice(coeff, arrived, (jnp.int32(0), before * width))
    rms = jnp.sqrt(blocks.sum(axis=(0, 1)) / total_rows)
    return (vec, coeff, rms)


def solution(mesh):
    placed = (P("row", "segment"), P("row", "segment"))
    return jax.shard_map(
        per_device,
        mesh=mesh,
        in_specs=placed,
        out_specs=(P("row", "segment"), P("segment", None), P("segment")),
        check_vma=False,
    )
```

```python
import jax
import jax.numpy as jnp
from jax import lax
from jax.experimental import pallas as pl
from jax.experimental.pallas import tpu as pltpu
from jax.sharding import PartitionSpec as P


TILE = 128
NEAR = 8


def exchange(blocks, axis, groups=None):
    return lax.all_to_all(
        blocks, axis, split_axis=0, concat_axis=0, axis_index_groups=groups, tiled=True
    )


def rings(axis):
    count = lax.axis_size(axis)
    near = [[a + b for b in range(NEAR)] for a in range(0, count, NEAR)]
    far = [[a + b for a in range(0, count, NEAR)] for b in range(NEAR)]
    return near, far


def gathered(mine, near, far):
    blocks = exchange(mine.reshape(len(far[0]), -1, TILE), "row", far)
    own = blocks.sum(axis=0)
    blocks = exchange(jnp.broadcast_to(own, blocks.shape), "row", far).reshape(-1, TILE)
    blocks = exchange(jnp.broadcast_to(blocks, (len(near[0]), *blocks.shape)), "row", near)
    return blocks.reshape(-1, TILE)


def shifted(value, axis, steps):
    count = lax.axis_size(axis)
    pairs = [(source, (source + steps) % count) for source in range(count)]
    return lax.ppermute(value, axis, pairs)


def halves(value):
    high = value.astype(jnp.bfloat16)
    return high, (value - high.astype(jnp.float32)).astype(jnp.bfloat16)


def product(a, b):
    def once(x, y):
        return jnp.dot(x, y, preferred_element_type=jnp.float32)

    return once(a[0], b[0]) + (once(a[0], b[1]) + once(a[1], b[0]))


def narrow_product(a, b):
    width = b[0].shape[1]
    wide = jnp.dot(a[0], jnp.concatenate(b, axis=1), preferred_element_type=jnp.float32)
    low = jnp.dot(a[1], b[0], preferred_element_type=jnp.float32)
    return wide[:, :width] + (wide[:, width:] + low)


def tiles_of(size):
    count = size // TILE
    return [(i, j) for i in range(count) for j in range(i, count)]


def start_kernel(basis_hbm, vec_hbm, out_ref, basis_ref, vec_ref, done):
    copies = [
        pltpu.make_async_copy(basis_hbm, basis_ref, done.at[0]),
        pltpu.make_async_copy(vec_hbm, vec_ref, done.at[1]),
    ]
    for copy in copies:
        copy.start()
    for copy in copies:
        copy.wait()
    basis = basis_ref[...]
    size = basis.shape[1]
    count = size // TILE
    turned = halves(basis.T)
    right = halves(jnp.concatenate([basis, vec_ref[...]], axis=1))
    at = 0
    for i in range(count):
        left = tuple(part[i * TILE:(i + 1) * TILE] for part in turned)
        strip = product(left, tuple(part[:, i * TILE:] for part in right))
        for j in range(count - i):
            out_ref[at:at + TILE] = strip[:, j * TILE:(j + 1) * TILE]
            at += TILE
        base = (len(tiles_of(size)) + i) * TILE
        out_ref[base:base + TILE] = strip[:, (count - i) * TILE:]


def both(first, gram_ref, size):
    count = size // TILE
    part = {}
    for at, (i, j) in enumerate(tiles_of(size)):
        tile = gram_ref[at * TILE:(at + 1) * TILE]
        part[i, j] = tile
        if i != j:
            part[j, i] = tile.T
    right = halves(first)
    rows = []
    for i in range(count):
        row = jnp.concatenate([part[i, j] for j in range(count)], axis=1)
        rows.append(narrow_product(halves(row), right))
    return 2.0 * first - jnp.concatenate(rows, axis=0)


def turn_kernel(got_ref, basis_ref, vec_ref, next_ref, here_ref, vec_out, first_out):
    size = basis_ref.shape[1]
    here = both(got_ref[got_ref.shape[0] - size:], got_ref, size)
    here_ref[...] = here
    vec = vec_ref[...] - narrow_product(halves(basis_ref[...]), halves(here))
    vec_out[...] = vec
    first_out[...] = narrow_product(halves(next_ref[...].T), halves(vec))


def end_kernel(first_ref, gram_ref, basis_ref, vec_ref, there_ref, vec_out, squares_ref):
    there = both(first_ref[...], gram_ref, basis_ref.shape[1])
    there_ref[...] = there
    vec = vec_ref[...] - narrow_product(halves(basis_ref[...]), halves(there))
    vec_out[...] = vec
    squares = jnp.sum(vec * vec, axis=0, keepdims=True)
    squares_ref[...] = jnp.broadcast_to(squares[None], squares_ref.shape)


def local(kernel, ins, outs, scratch=()):
    return pl.pallas_call(
        kernel,
        in_specs=[pl.BlockSpec(memory_space=space) for space in ins],
        out_specs=[pl.BlockSpec(memory_space=space) for space, _ in outs],
        out_shape=[jax.ShapeDtypeStruct(shape, jnp.float32) for _, shape in outs],
        scratch_shapes=scratch,
        compiler_params=pltpu.CompilerParams(vmem_limit_bytes=16 * 2**20),
    )


def per_device(snapshots, basis):
    sections = lax.axis_size("segment")
    lines = lax.axis_size("row")
    position = lax.axis_index("segment")
    rows, width = snapshots.shape
    size = basis.shape[1]
    share = len(tiles_of(size)) * TILE
    total_rows = rows * lines
    hbm = pltpu.HBM
    near, far = rings("row")

    onward = shifted(basis, "segment", -1)
    (sent,) = local(
        start_kernel, (hbm, hbm), [(pltpu.VMEM, (share + size, TILE))],
        (pltpu.VMEM(basis.shape, jnp.float32), pltpu.VMEM(snapshots.shape, jnp.float32),
         pltpu.SemaphoreType.DMA((2,))),
    )(*(pltpu.with_memory_space_constraint(array, hbm) for array in (basis, snapshots)))
    blocks = exchange(sent.reshape(len(near[0]), -1, TILE), "row", near)
    mine, onward = lax.optimization_barrier((blocks.sum(axis=0), onward))
    got = gathered(mine, near, far)
    gram_next = shifted(got[:share], "segment", -1)
    here, vec, first = local(
        turn_kernel, (pltpu.VMEM,) * 4,
        [(pltpu.VMEM, (size, width)), (pltpu.VMEM, (rows, width)), (pltpu.VMEM, (size, width))],
    )(got, basis, snapshots, onward)
    coeff = jnp.zeros((size, width * sections), jnp.float32)
    coeff = lax.dynamic_update_slice(coeff, here, (jnp.int32(0), position * width))
    blocks = exchange(first.reshape(lines, -1, TILE), "row")
    mine, coeff = lax.optimization_barrier((blocks.sum(axis=0), coeff))
    first = exchange(jnp.broadcast_to(mine, blocks.shape), "row")
    first = lax.optimization_barrier(first)
    first, gram_next = lax.optimization_barrier((first, gram_next))
    there, vec, squares = local(
        end_kernel, (pltpu.VMEM,) * 4,
        [(pltpu.VMEM, (size, width)), (pltpu.VMEM, (rows, width)),
         (pltpu.VMEM, (lines, 1, width))],
    )(first.reshape(-1, TILE), gram_next, onward, vec)

    arrived = shifted(there, "segment", 1)
    blocks = exchange(squares, "row")
    before = (position - 1) % sections
    coeff = lax.dynamic_update_slice(coeff, arrived, (jnp.int32(0), before * width))
    rms = jnp.sqrt(blocks.sum(axis=(0, 1)) / total_rows)
    return (vec, coeff, rms)


def solution(mesh):
    placed = (P("row", "segment"), P("row", "segment"))
    return jax.shard_map(
        per_device,
        mesh=mesh,
        in_specs=placed,
        out_specs=(P("row", "segment"), P("segment", None), P("segment")),
        check_vma=False,
    )
```

```python
import jax
import jax.numpy as jnp
from jax import lax
from jax.experimental import pallas as pl
from jax.experimental.pallas import tpu as pltpu
from jax.sharding import PartitionSpec as P


TILE = 128
NEAR = 16


def exchange(blocks, axis, groups=None):
    return lax.all_to_all(
        blocks, axis, split_axis=0, concat_axis=0, axis_index_groups=groups, tiled=True
    )


def rings(axis):
    count = lax.axis_size(axis)
    near = [[a + b for b in range(NEAR)] for a in range(0, count, NEAR)]
    far = [[a + b for a in range(0, count, NEAR)] for b in range(NEAR)]
    return near, far


def gathered(mine, near, far):
    blocks = exchange(jnp.broadcast_to(mine, (len(far[0]), *mine.shape)), "row", far)
    own = blocks.sum(axis=0)
    blocks = exchange(jnp.broadcast_to(own, (len(near[0]), *own.shape)), "row", near)
    return blocks.reshape(-1, TILE)


def shifted(value, axis, steps):
    count = lax.axis_size(axis)
    pairs = [(source, (source + steps) % count) for source in range(count)]
    return lax.ppermute(value, axis, pairs)


def halves(value):
    high = value.astype(jnp.bfloat16)
    return high, (value - high.astype(jnp.float32)).astype(jnp.bfloat16)


def product(a, b):
    def once(x, y):
        return jnp.dot(x, y, preferred_element_type=jnp.float32)

    return once(a[0], b[0]) + (once(a[0], b[1]) + once(a[1], b[0]))


def narrow_product(a, b):
    width = b[0].shape[1]
    wide = jnp.dot(a[0], jnp.concatenate(b, axis=1), preferred_element_type=jnp.float32)
    low = jnp.dot(a[1], b[0], preferred_element_type=jnp.float32)
    return wide[:, :width] + (wide[:, width:] + low)


def tiles_of(size):
    count = size // TILE
    return [(i, j) for i in range(count) for j in range(i, count)]


def start_kernel(basis_hbm, vec_hbm, out_ref, basis_ref, vec_ref, done):
    copies = [
        pltpu.make_async_copy(basis_hbm, basis_ref, done.at[0]),
        pltpu.make_async_copy(vec_hbm, vec_ref, done.at[1]),
    ]
    for copy in copies:
        copy.start()
    for copy in copies:
        copy.wait()
    basis = basis_ref[...]
    size = basis.shape[1]
    count = size // TILE
    turned = halves(basis.T)
    right = halves(jnp.concatenate([basis, vec_ref[...]], axis=1))
    at = 0
    for i in range(count):
        left = tuple(part[i * TILE:(i + 1) * TILE] for part in turned)
        strip = product(left, tuple(part[:, i * TILE:] for part in right))
        for j in range(count - i):
            out_ref[at:at + TILE] = strip[:, j * TILE:(j + 1) * TILE]
            at += TILE
        base = (len(tiles_of(size)) + i) * TILE
        out_ref[base:base + TILE] = strip[:, (count - i) * TILE:]


def both(first, gram_ref, size):
    count = size // TILE
    part = {}
    for at, (i, j) in enumerate(tiles_of(size)):
        tile = gram_ref[at * TILE:(at + 1) * TILE]
        part[i, j] = tile
        if i != j:
            part[j, i] = tile.T
    right = halves(first)
    rows = []
    for i in range(count):
        row = jnp.concatenate([part[i, j] for j in range(count)], axis=1)
        rows.append(narrow_product(halves(row), right))
    return 2.0 * first - jnp.concatenate(rows, axis=0)


def turn_kernel(got_ref, basis_ref, vec_ref, next_ref, here_ref, vec_out, first_out):
    size = basis_ref.shape[1]
    here = both(got_ref[got_ref.shape[0] - size:], got_ref, size)
    here_ref[...] = here
    vec = vec_ref[...] - narrow_product(halves(basis_ref[...]), halves(here))
    vec_out[...] = vec
    first_out[...] = narrow_product(halves(next_ref[...].T), halves(vec))


def end_kernel(first_ref, gram_ref, basis_ref, vec_ref, there_ref, vec_out, squares_ref):
    there = both(first_ref[...], gram_ref, basis_ref.shape[1])
    there_ref[...] = there
    vec = vec_ref[...] - narrow_product(halves(basis_ref[...]), halves(there))
    vec_out[...] = vec
    squares = jnp.sum(vec * vec, axis=0, keepdims=True)
    squares_ref[...] = jnp.broadcast_to(squares[None], squares_ref.shape)


def local(kernel, ins, outs, scratch=()):
    return pl.pallas_call(
        kernel,
        in_specs=[pl.BlockSpec(memory_space=space) for space in ins],
        out_specs=[pl.BlockSpec(memory_space=space) for space, _ in outs],
        out_shape=[jax.ShapeDtypeStruct(shape, jnp.float32) for _, shape in outs],
        scratch_shapes=scratch,
        compiler_params=pltpu.CompilerParams(vmem_limit_bytes=16 * 2**20),
    )


def per_device(snapshots, basis):
    sections = lax.axis_size("segment")
    lines = lax.axis_size("row")
    position = lax.axis_index("segment")
    rows, width = snapshots.shape
    size = basis.shape[1]
    share = len(tiles_of(size)) * TILE
    total_rows = rows * lines
    hbm = pltpu.HBM
    near, far = rings("row")

    onward = shifted(basis, "segment", -1)
    (sent,) = local(
        start_kernel, (hbm, hbm), [(pltpu.VMEM, (share + size, TILE))],
        (pltpu.VMEM(basis.shape, jnp.float32), pltpu.VMEM(snapshots.shape, jnp.float32),
         pltpu.SemaphoreType.DMA((2,))),
    )(*(pltpu.with_memory_space_constraint(array, hbm) for array in (basis, snapshots)))
    blocks = exchange(sent.reshape(len(near[0]), -1, TILE), "row", near)
    mine, onward = lax.optimization_barrier((blocks.sum(axis=0), onward))
    got = gathered(mine, near, far)
    gram_next = shifted(got[:share], "segment", -1)
    here, vec, first = local(
        turn_kernel, (pltpu.VMEM,) * 4,
        [(pltpu.VMEM, (size, width)), (pltpu.VMEM, (rows, width)), (pltpu.VMEM, (size, width))],
    )(got, basis, snapshots, onward)
    coeff = jnp.zeros((size, width * sections), jnp.float32)
    coeff = lax.dynamic_update_slice(coeff, here, (jnp.int32(0), position * width))
    blocks = exchange(first.reshape(lines, -1, TILE), "row")
    mine, coeff = lax.optimization_barrier((blocks.sum(axis=0), coeff))
    first = exchange(jnp.broadcast_to(mine, blocks.shape), "row")
    first = lax.optimization_barrier(first)
    first, gram_next = lax.optimization_barrier((first, gram_next))
    there, vec, squares = local(
        end_kernel, (pltpu.VMEM,) * 4,
        [(pltpu.VMEM, (size, width)), (pltpu.VMEM, (rows, width)),
         (pltpu.VMEM, (lines, 1, width))],
    )(first.reshape(-1, TILE), gram_next, onward, vec)

    arrived = shifted(there, "segment", 1)
    blocks = exchange(squares, "row")
    before = (position - 1) % sections
    coeff = lax.dynamic_update_slice(coeff, arrived, (jnp.int32(0), before * width))
    rms = jnp.sqrt(blocks.sum(axis=(0, 1)) / total_rows)
    return (vec, coeff, rms)


def solution(mesh):
    placed = (P("row", "segment"), P("row", "segment"))
    return jax.shard_map(
        per_device,
        mesh=mesh,
        in_specs=placed,
        out_specs=(P("row", "segment"), P("segment", None), P("segment")),
        check_vma=False,
    )
```

```python
import jax
import jax.numpy as jnp
from jax import lax
from jax.experimental import pallas as pl
from jax.experimental.pallas import tpu as pltpu
from jax.sharding import PartitionSpec as P


TILE = 128
NEAR = 8


def exchange(blocks, axis, groups=None):
    return lax.all_to_all(
        blocks, axis, split_axis=0, concat_axis=0, axis_index_groups=groups, tiled=True
    )


def rings(axis):
    count = lax.axis_size(axis)
    near = [[a + b for b in range(NEAR)] for a in range(0, count, NEAR)]
    far = [[a + b for a in range(0, count, NEAR)] for b in range(NEAR)]
    return near, far


def gathered(mine, near, far):
    blocks = exchange(jnp.broadcast_to(mine, (len(far[0]), *mine.shape)), "row", far)
    own = blocks.sum(axis=0)
    blocks = exchange(jnp.broadcast_to(own, (len(near[0]), *own.shape)), "row", near)
    return blocks.reshape(-1, TILE)


def shifted(value, axis, steps):
    count = lax.axis_size(axis)
    pairs = [(source, (source + steps) % count) for source in range(count)]
    return lax.ppermute(value, axis, pairs)


def halves(value):
    high = value.astype(jnp.bfloat16)
    return high, (value - high.astype(jnp.float32)).astype(jnp.bfloat16)


def product(a, b):
    def once(x, y):
        return jnp.dot(x, y, preferred_element_type=jnp.float32)

    return once(a[0], b[0]) + (once(a[0], b[1]) + once(a[1], b[0]))


def narrow_product(a, b):
    width = b[0].shape[1]
    wide = jnp.dot(a[0], jnp.concatenate(b, axis=1), preferred_element_type=jnp.float32)
    low = jnp.dot(a[1], b[0], preferred_element_type=jnp.float32)
    return wide[:, :width] + (wide[:, width:] + low)


def tiles_of(size):
    count = size // TILE
    return [(i, j) for i in range(count) for j in range(i, count)]


def start_kernel(basis_hbm, vec_hbm, out_ref, basis_ref, vec_ref, done):
    copies = [
        pltpu.make_async_copy(basis_hbm, basis_ref, done.at[0]),
        pltpu.make_async_copy(vec_hbm, vec_ref, done.at[1]),
    ]
    for copy in copies:
        copy.start()
    for copy in copies:
        copy.wait()
    basis = basis_ref[...]
    size = basis.shape[1]
    count = size // TILE
    turned = halves(basis.T)
    right = halves(jnp.concatenate([basis, vec_ref[...]], axis=1))
    at = 0
    for i in range(count):
        left = tuple(part[i * TILE:(i + 1) * TILE] for part in turned)
        strip = product(left, tuple(part[:, i * TILE:] for part in right))
        for j in range(count - i):
            out_ref[at:at + TILE] = strip[:, j * TILE:(j + 1) * TILE]
            at += TILE
        base = (len(tiles_of(size)) + i) * TILE
        out_ref[base:base + TILE] = strip[:, (count - i) * TILE:]


def both(first, gram_ref, size):
    count = size // TILE
    part = {}
    for at, (i, j) in enumerate(tiles_of(size)):
        tile = gram_ref[at * TILE:(at + 1) * TILE]
        part[i, j] = tile
        if i != j:
            part[j, i] = tile.T
    right = halves(first)
    rows = []
    for i in range(count):
        row = jnp.concatenate([part[i, j] for j in range(count)], axis=1)
        rows.append(narrow_product(halves(row), right))
    return 2.0 * first - jnp.concatenate(rows, axis=0)


def turn_kernel(got_ref, basis_ref, vec_ref, next_ref, here_ref, vec_out, first_out):
    size = basis_ref.shape[1]
    here = both(got_ref[got_ref.shape[0] - size:], got_ref, size)
    here_ref[...] = here
    vec = vec_ref[...] - narrow_product(halves(basis_ref[...]), halves(here))
    vec_out[...] = vec
    first_out[...] = narrow_product(halves(next_ref[...].T), halves(vec))


def end_kernel(first_ref, gram_ref, basis_ref, vec_ref, there_ref, vec_out, squares_ref):
    there = both(first_ref[...], gram_ref, basis_ref.shape[1])
    there_ref[...] = there
    vec = vec_ref[...] - narrow_product(halves(basis_ref[...]), halves(there))
    vec_out[...] = vec
    squares = jnp.sum(vec * vec, axis=0, keepdims=True)
    squares_ref[...] = jnp.broadcast_to(squares[None], squares_ref.shape)


def local(kernel, ins, outs, scratch=()):
    return pl.pallas_call(
        kernel,
        in_specs=[pl.BlockSpec(memory_space=space) for space in ins],
        out_specs=[pl.BlockSpec(memory_space=space) for space, _ in outs],
        out_shape=[jax.ShapeDtypeStruct(shape, jnp.float32) for _, shape in outs],
        scratch_shapes=scratch,
        compiler_params=pltpu.CompilerParams(vmem_limit_bytes=16 * 2**20),
    )


def per_device(snapshots, basis):
    sections = lax.axis_size("segment")
    lines = lax.axis_size("row")
    position = lax.axis_index("segment")
    rows, width = snapshots.shape
    size = basis.shape[1]
    share = len(tiles_of(size)) * TILE
    total_rows = rows * lines
    hbm = pltpu.HBM
    near, far = rings("row")

    onward = shifted(basis, "segment", -1)
    (sent,) = local(
        start_kernel, (hbm, hbm), [(pltpu.VMEM, (share + size, TILE))],
        (pltpu.VMEM(basis.shape, jnp.float32), pltpu.VMEM(snapshots.shape, jnp.float32),
         pltpu.SemaphoreType.DMA((2,))),
    )(*(pltpu.with_memory_space_constraint(array, hbm) for array in (basis, snapshots)))
    blocks = exchange(sent.reshape(len(near[0]), -1, TILE), "row", near)
    mine, onward = lax.optimization_barrier((blocks.sum(axis=0), onward))
    got = gathered(mine, near, far)
    gram_next = shifted(got[:share], "segment", -1)
    here, vec, first = local(
        turn_kernel, (pltpu.VMEM,) * 4,
        [(pltpu.VMEM, (size, width)), (pltpu.VMEM, (rows, width)), (pltpu.VMEM, (size, width))],
    )(got, basis, snapshots, onward)
    coeff = jnp.zeros((size, width * sections), jnp.float32)
    coeff = lax.dynamic_update_slice(coeff, here, (jnp.int32(0), position * width))
    blocks = exchange(first.reshape(len(near[0]), -1, TILE), "row", near)
    first = gathered(blocks.sum(axis=0), near, far)
    first = lax.optimization_barrier(first)
    first, gram_next = lax.optimization_barrier((first, gram_next))
    there, vec, squares = local(
        end_kernel, (pltpu.VMEM,) * 4,
        [(pltpu.VMEM, (size, width)), (pltpu.VMEM, (rows, width)),
         (pltpu.VMEM, (lines, 1, width))],
    )(first.reshape(-1, TILE), gram_next, onward, vec)

    arrived = shifted(there, "segment", 1)
    blocks = exchange(squares, "row")
    before = (position - 1) % sections
    coeff = lax.dynamic_update_slice(coeff, arrived, (jnp.int32(0), before * width))
    rms = jnp.sqrt(blocks.sum(axis=(0, 1)) / total_rows)
    return (vec, coeff, rms)


def solution(mesh):
    placed = (P("row", "segment"), P("row", "segment"))
    return jax.shard_map(
        per_device,
        mesh=mesh,
        in_specs=placed,
        out_specs=(P("row", "segment"), P("segment", None), P("segment")),
        check_vma=False,
    )
```

```python
import jax
import jax.numpy as jnp
from jax import lax
from jax.experimental import pallas as pl
from jax.experimental.pallas import tpu as pltpu
from jax.sharding import PartitionSpec as P


TILE = 128
NEAR = 8


def exchange(blocks, axis, groups=None):
    return lax.all_to_all(
        blocks, axis, split_axis=0, concat_axis=0, axis_index_groups=groups, tiled=True
    )


def rings(axis):
    count = lax.axis_size(axis)
    near = [[a + b for b in range(NEAR)] for a in range(0, count, NEAR)]
    far = [[a + b for a in range(0, count, NEAR)] for b in range(NEAR)]
    return near, far


def gathered(mine, near, far):
    blocks = exchange(jnp.broadcast_to(mine, (len(far[0]), *mine.shape)), "row", far)
    own = blocks.sum(axis=0)
    blocks = exchange(jnp.broadcast_to(own, (len(near[0]), *own.shape)), "row", near)
    return blocks.reshape(-1, TILE)


def shifted(value, axis, steps):
    count = lax.axis_size(axis)
    pairs = [(source, (source + steps) % count) for source in range(count)]
    return lax.ppermute(value, axis, pairs)


def halves(value):
    high = value.astype(jnp.bfloat16)
    return high, (value - high.astype(jnp.float32)).astype(jnp.bfloat16)


def product(a, b):
    def once(x, y):
        return jnp.dot(x, y, preferred_element_type=jnp.float32)

    return once(a[0], b[0]) + (once(a[0], b[1]) + once(a[1], b[0]))


def narrow_product(a, b):
    width = b[0].shape[1]
    wide = jnp.dot(a[0], jnp.concatenate(b, axis=1), preferred_element_type=jnp.float32)
    low = jnp.dot(a[1], b[0], preferred_element_type=jnp.float32)
    return wide[:, :width] + (wide[:, width:] + low)


def tiles_of(size):
    count = size // TILE
    return [(i, j) for i in range(count) for j in range(i, count)]


def start_kernel(basis_hbm, vec_hbm, out_ref, basis_ref, vec_ref, done):
    copies = [
        pltpu.make_async_copy(basis_hbm, basis_ref, done.at[0]),
        pltpu.make_async_copy(vec_hbm, vec_ref, done.at[1]),
    ]
    for copy in copies:
        copy.start()
    for copy in copies:
        copy.wait()
    basis = basis_ref[...]
    size = basis.shape[1]
    count = size // TILE
    turned = halves(basis.T)
    right = halves(jnp.concatenate([basis, vec_ref[...]], axis=1))
    at = 0
    for i in range(count):
        left = tuple(part[i * TILE:(i + 1) * TILE] for part in turned)
        strip = product(left, tuple(part[:, i * TILE:] for part in right))
        for j in range(count - i):
            out_ref[at:at + TILE] = strip[:, j * TILE:(j + 1) * TILE]
            at += TILE
        base = (len(tiles_of(size)) + i) * TILE
        out_ref[base:base + TILE] = strip[:, (count - i) * TILE:]


def both(first, gram_ref, size):
    count = size // TILE
    part = {}
    for at, (i, j) in enumerate(tiles_of(size)):
        tile = gram_ref[at * TILE:(at + 1) * TILE]
        part[i, j] = tile
        if i != j:
            part[j, i] = tile.T
    right = halves(first)
    rows = []
    for i in range(count):
        row = jnp.concatenate([part[i, j] for j in range(count)], axis=1)
        rows.append(narrow_product(halves(row), right))
    return 2.0 * first - jnp.concatenate(rows, axis=0)


def turn_kernel(got_ref, basis_ref, vec_ref, next_ref, here_ref, vec_out, first_out):
    size = basis_ref.shape[1]
    here = both(got_ref[got_ref.shape[0] - size:], got_ref, size)
    here_ref[...] = here
    vec = vec_ref[...] - narrow_product(halves(basis_ref[...]), halves(here))
    vec_out[...] = vec
    first_out[...] = narrow_product(halves(next_ref[...].T), halves(vec))


def end_kernel(first_ref, gram_ref, basis_ref, vec_ref, there_ref, vec_out, squares_ref):
    there = both(first_ref[...], gram_ref, basis_ref.shape[1])
    there_ref[...] = there
    vec = vec_ref[...] - narrow_product(halves(basis_ref[...]), halves(there))
    vec_out[...] = vec
    squares = jnp.sum(vec * vec, axis=0, keepdims=True)
    squares_ref[...] = jnp.broadcast_to(squares[None], squares_ref.shape)


def local(kernel, ins, outs, scratch=()):
    return pl.pallas_call(
        kernel,
        in_specs=[pl.BlockSpec(memory_space=space) for space in ins],
        out_specs=[pl.BlockSpec(memory_space=space) for space, _ in outs],
        out_shape=[jax.ShapeDtypeStruct(shape, jnp.float32) for _, shape in outs],
        scratch_shapes=scratch,
        compiler_params=pltpu.CompilerParams(vmem_limit_bytes=16 * 2**20),
    )


def per_device(snapshots, basis):
    sections = lax.axis_size("segment")
    lines = lax.axis_size("row")
    position = lax.axis_index("segment")
    rows, width = snapshots.shape
    size = basis.shape[1]
    share = len(tiles_of(size)) * TILE
    total_rows = rows * lines
    hbm = pltpu.HBM
    near, far = rings("row")

    onward = shifted(basis, "segment", -1)
    (sent,) = local(
        start_kernel, (hbm, hbm), [(pltpu.VMEM, (share + size, TILE))],
        (pltpu.VMEM(basis.shape, jnp.float32), pltpu.VMEM(snapshots.shape, jnp.float32),
         pltpu.SemaphoreType.DMA((2,))),
    )(*(pltpu.with_memory_space_constraint(array, hbm) for array in (basis, snapshots)))
    blocks = exchange(sent.reshape(len(near[0]), -1, TILE), "row", near)
    mine, onward = lax.optimization_barrier((blocks.sum(axis=0), onward))
    got = gathered(mine, near, far)
    gram_next = shifted(got[:share], "segment", -1)
    here, vec, first = local(
        turn_kernel, (pltpu.VMEM,) * 4,
        [(pltpu.VMEM, (size, width)), (pltpu.VMEM, (rows, width)), (pltpu.VMEM, (size, width))],
    )(got, basis, snapshots, onward)
    blocks = exchange(first.reshape(len(near[0]), -1, TILE), "row", near)
    mine = blocks.sum(axis=0)
    blocks = exchange(jnp.broadcast_to(mine, (len(far[0]), *mine.shape)), "row", far)
    before = (position - 1) % sections
    own, at, behind = lax.optimization_barrier(
        (blocks.sum(axis=0), position * width, before * width)
    )
    first = exchange(jnp.broadcast_to(own, (len(near[0]), *own.shape)), "row", near)
    first = lax.optimization_barrier(first)
    first, gram_next = lax.optimization_barrier((first, gram_next))
    there, vec, squares = local(
        end_kernel, (pltpu.VMEM,) * 4,
        [(pltpu.VMEM, (size, width)), (pltpu.VMEM, (rows, width)),
         (pltpu.VMEM, (lines, 1, width))],
    )(first.reshape(-1, TILE), gram_next, onward, vec)

    arrived = shifted(there, "segment", 1)
    blocks = exchange(squares, "row")
    coeff = jnp.zeros((size, width * sections), jnp.float32)
    coeff = lax.dynamic_update_slice(coeff, here, (jnp.int32(0), at))
    coeff = lax.dynamic_update_slice(coeff, arrived, (jnp.int32(0), behind))
    rms = jnp.sqrt(blocks.sum(axis=(0, 1)) / total_rows)
    return (vec, coeff, rms)


def solution(mesh):
    placed = (P("row", "segment"), P("row", "segment"))
    return jax.shard_map(
        per_device,
        mesh=mesh,
        in_specs=placed,
        out_specs=(P("row", "segment"), P("segment", None), P("segment")),
        check_vma=False,
    )
```
